32 devices in a mesh: pr: 4 (over y, x), pc: 8 (over z, core).
Axes of the slice: x: 2, y: 2, z: 4, core: 2. Of those that a mesh axis runs over, the one named last changes fastest.
Arguments:
- pair_state: bfloat16 [96, 96, 128], P('pr', 'pc'), may hold values from -6 to 6
- left_weight: bfloat16 [128, 128], replicated, may hold values from -0.5 to 0.5
- right_weight: bfloat16 [128, 128], replicated, may hold values from -0.5 to 0.5
- mid_gain: float32 [128], replicated, may hold values from 0.25 to 1.75
- out_weight: bfloat16 [128, 128], replicated, may hold values from -0.5 to 0.5
- out_gate: bfloat16 [128, 128], replicated, may hold values from -0.5 to 0.5
Outputs:
- pair_update: bfloat16 [96, 96, 128], P('pr', 'pc')
The draws below stay inside these ranges and needn't reach their ends.
All inputs are finite; a program needn't handle non-finite values.
Results may differ from the reference program's by a relative error of at most 0.012.
Values may be sent and summed in bfloat16 or wider, within the bound.
A program may use at most 128 MiB of HBM per device.

```python
import jax
import jax.numpy as jnp
from jax import lax

RESIDUES = 96
PAIR_WIDTH = 128
MIX_WIDTH = 128


def levels(stream_key, dims, pieces, smallest, top_value):
    level, own = 1.0, jax.random.fold_in(stream_key, 6)
    for dim, shards_of in pieces:
        heights = jnp.exp(jax.random.uniform(jax.random.fold_in(own, dim), (shards_of,), jnp.float32, smallest / len(pieces), top_value / len(pieces)))
        level = level * jnp.repeat(heights, dims[dim] // shards_of).reshape([-1 if axis == dim else 1 for axis in range(len(dims))])
    return level


def scatter_about(key, shape, spread, limit, shards=(), kind=jnp.bfloat16):
    array = spread * jax.random.normal(key, shape, jnp.float32)
    if shards:
        array = array * levels(key, shape, shards, -0.22, 0.18)
    return jnp.clip(array, -limit, limit).astype(kind)


def setup_inputs(seed: int = 0) -> dict:
    keys = jax.random.split(jax.random.key(seed), 7)
    pair_state = scatter_about(keys[0], (RESIDUES, RESIDUES, PAIR_WIDTH), 1.0, 6.0, ((0, 4), (1, 8)))
    left_weight = scatter_about(keys[1], (PAIR_WIDTH, MIX_WIDTH), PAIR_WIDTH ** -0.5, 0.5)
    right_weight = scatter_about(keys[2], (PAIR_WIDTH, MIX_WIDTH), PAIR_WIDTH ** -0.5, 0.5)
    mid_gain = jnp.clip(1.0 + 0.15 * jax.random.normal(keys[3], (MIX_WIDTH,), jnp.float32), 0.25, 1.75)
    out_weight = scatter_about(keys[4], (MIX_WIDTH, PAIR_WIDTH), MIX_WIDTH ** -0.5, 0.5)
    out_gate = scatter_about(keys[5], (PAIR_WIDTH, PAIR_WIDTH), PAIR_WIDTH ** -0.5, 0.5)
    return dict(pair_state=pair_state, left_weight=left_weight, right_weight=right_weight, mid_gain=mid_gain, out_weight=out_weight, out_gate=out_gate)


def scale_channels(values, channel_gain):
    centred = values - lax.optimization_barrier(jnp.mean(values, axis=-1, keepdims=True))
    return centred * lax.rsqrt(lax.optimization_barrier(jnp.mean(centred * centred, axis=-1, keepdims=True)) + 1e-05) * channel_gain

def project_pair(pair_in, left_weight, right_weight):
    ready = pair_in
    left = jnp.einsum('ijc,cd->ijd', ready.astype(jnp.float32), left_weight.astype(jnp.float32))
    right = jnp.einsum('ijc,cd->ijd', ready.astype(jnp.float32), right_weight.astype(jnp.float32))
    return (ready, left.astype(jnp.bfloat16), right.astype(jnp.bfloat16))

def close_update(mixed, ready, mid_gain, out_weight, out_gate):
    scaled = scale_channels(mixed.astype(jnp.float32), mid_gain).astype(jnp.bfloat16)
    scaled = lax.optimization_barrier(scaled)
    gate = jax.nn.sigmoid(jnp.einsum('ijc,cd->ijd', ready.astype(jnp.float32), out_gate.astype(jnp.float32)))
    return (jnp.einsum('ijd,dc->ijc', scaled.astype(jnp.float32), out_weight.astype(jnp.float32)) * gate).astype(jnp.bfloat16)

def reference(pair_state, left_weight, right_weight, mid_gain, out_weight, out_gate):
    ready, left, right = project_pair(pair_state, left_weight, right_weight)
    left, right = lax.optimization_barrier((left, right))

    def one_channel(pair_of):
        return (jnp.dot(pair_of[0].T, pair_of[1], preferred_element_type=jnp.float32) * RESIDUES ** (-0.5)).astype(jnp.bfloat16)
    mixed = jnp.moveaxis(lax.map(one_channel, (jnp.moveaxis(left, -1, 0), jnp.moveaxis(right, -1, 0))), 0, -1)
    mixed = lax.optimization_barrier(mixed)
    return close_update(mixed, ready, mid_gain, out_weight, out_gate)
```

```python
import functools

import jax
import jax.numpy as jnp
from jax import lax
from jax.experimental import pallas as pl
from jax.experimental.pallas import tpu as pltpu
from jax.sharding import PartitionSpec as P

VMEM_LIMIT = 48 * 1024 * 1024
MESH = pl.DeviceIdType.MESH


def scale_channels(values, channel_gain):
    centred = values - jnp.mean(values, axis=-1, keepdims=True)
    return (
        centred
        * lax.rsqrt(jnp.mean(centred * centred, axis=-1, keepdims=True) + 1e-05)
        * channel_gain
    )


def project_pair(pair_in, left_weight, right_weight):
    left = jnp.einsum("ijc,cd->ijd", pair_in, left_weight, preferred_element_type=jnp.float32)
    right = jnp.einsum("ijc,cd->ijd", pair_in, right_weight, preferred_element_type=jnp.float32)
    return (pair_in, left.astype(jnp.bfloat16), right.astype(jnp.bfloat16))


def close_update(mixed, ready, mid_gain, out_weight, out_gate):
    scaled = scale_channels(mixed.astype(jnp.float32), mid_gain).astype(jnp.bfloat16)
    scaled = lax.optimization_barrier(scaled)
    gate = jax.nn.sigmoid(
        jnp.einsum("ijc,cd->ijd", ready, out_gate, preferred_element_type=jnp.float32)
    )
    return (
        jnp.einsum("ijd,dc->ijc", scaled, out_weight, preferred_element_type=jnp.float32) * gate
    ).astype(jnp.bfloat16)


def plain_body(pair_state, left_weight, right_weight, mid_gain, out_weight, out_gate):
    ready, left, right = project_pair(pair_state, left_weight, right_weight)
    count = pair_state.shape[0] * lax.axis_size("pr")
    left_lines, right_lines = (
        lax.all_to_all(left, "pr", split_axis=2, concat_axis=0, tiled=True),
        lax.all_to_all(right, "pr", split_axis=2, concat_axis=0, tiled=True),
    )
    strip = jnp.einsum(
        "kid,kjd->ijd",
        lax.all_gather(left_lines, "pc", axis=1, tiled=True),
        right_lines,
        preferred_element_type=jnp.float32,
    )
    strip = (strip * count ** (-0.5)).astype(jnp.bfloat16)
    mixed = lax.all_to_all(strip, "pr", split_axis=0, concat_axis=2, tiled=True)
    return close_update(mixed, ready, mid_gain, out_weight, out_gate)


def pick(table, index):
    value = jnp.int32(table[0])
    for place in range(1, len(table)):
        value = jnp.where(index == place, jnp.int32(table[place]), value)
    return value


def kernel(
    rows_of, line_of,
    x_hbm, wl_hbm, wr_hbm, gain_hbm, wo_hbm, wg_hbm, o_ref,
    xv, wl, wr, gain, wo, wg, flat, xf, xsib, zbuf, lbuf, rbuf, gate, pout, pin,
    in_sem, x_send, x_recv, z_send, z_recv, p_send, p_recv,
):
    K, J, D = xv.shape
    N = K * J
    half = J * J
    a = lax.axis_index("pr")
    c = lax.axis_index("pc")
    z, core = c // 2, c % 2
    sib = c + 1 - 2 * core
    order = [
        pick([sorted((o for o in range(line_of) if o != m), key=lambda o: abs(o - m))[t] for m in range(line_of)], z)
        for t in range(line_of - 1)
    ]

    barrier = pltpu.get_barrier_semaphore()
    loads = [
        pltpu.make_async_copy(s, d, in_sem.at[n])
        for n, (s, d) in enumerate(
            ((x_hbm, xv), (wr_hbm, wr), (wl_hbm, wl), (wg_hbm, wg), (gain_hbm, gain), (wo_hbm, wo))
        )
    ]
    for load in loads:
        load.start()
    for other in order:
        pl.semaphore_signal(barrier, inc=1, device_id=(a, other * 2 + core), device_id_type=MESH)
    pl.semaphore_signal(barrier, inc=1, device_id=(a, sib), device_id_type=MESH)
    for step in range(1, rows_of):
        row = (a + step) % rows_of
        pl.semaphore_signal(barrier, inc=1, device_id=(row, c), device_id_type=MESH)
        pl.semaphore_signal(barrier, inc=1, device_id=(row, sib), device_id_type=MESH)

    loads[0].wait()
    for k in range(K):
        flat[k * J : (k + 1) * J, :] = xv[k].astype(jnp.float32)
    xf[...] = flat[...].astype(xf.dtype)
    pl.semaphore_wait(barrier, line_of - 1 + 1 + 2 * (rows_of - 1))

    to_sib = pltpu.make_async_remote_copy(
        src_ref=xf, dst_ref=xsib, send_sem=x_send, recv_sem=x_recv,
        device_id=(a, sib), device_id_type=MESH,
    )
    to_line = [
        pltpu.make_async_remote_copy(
            src_ref=xf, dst_ref=zbuf.at[z], send_sem=z_send.at[t], recv_sem=z_recv.at[z],
            device_id=(a, other * 2 + core), device_id_type=MESH,
        )
        for t, other in enumerate(order)
    ]
    for copy in to_line:
        copy.start()
    to_sib.start()

    for load in loads[1:]:
        load.wait()
    own = jnp.dot(xf[...], wr[...], preferred_element_type=jnp.float32)
    rbuf[:, :J, :] = own.reshape(K, J, D)
    lbuf[...] = jnp.dot(xf[...], wl[...], preferred_element_type=jnp.float32)
    gate[...] = jax.nn.sigmoid(jnp.dot(xf[...], wg[...], preferred_element_type=jnp.float32))
    to_sib.wait()
    other_right = jnp.dot(xsib[...], wr[...], preferred_element_type=jnp.float32)
    rbuf[:, J:, :] = other_right.reshape(K, J, D)

    sends = []
    for t in range(line_of):
        if t == 0:
            origin = z
        else:
            origin = order[t - 1]
            pltpu.make_async_copy(xf, zbuf.at[origin], z_recv.at[origin]).wait()
            lbuf[...] = jnp.dot(zbuf[origin], wl[...], preferred_element_type=jnp.float32)

        def step(k, sums):
            right = rbuf[k]
            return tuple(
                total + lbuf[pl.ds(k * J + i, 1), :] * right for i, total in enumerate(sums)
            )

        sums = lax.fori_loop(
            0, K, step, tuple(jnp.zeros((2 * J, D), jnp.float32) for _ in range(J)), unroll=2
        )
        for i in range(J):
            flat[i * J : (i + 1) * J, :] = sums[i][:J]
            flat[half + i * J : half + (i + 1) * J, :] = sums[i][J:]
        for h in range(2):
            pout[t, h] = flat[h * half : (h + 1) * half, :].astype(pout.dtype)
        away = pltpu.make_async_remote_copy(
            src_ref=pout.at[t, 0], dst_ref=pin.at[a, core], send_sem=p_send.at[t, 0],
            recv_sem=p_recv.at[a, core], device_id=(origin, c), device_id_type=MESH,
        )
        here = pltpu.make_async_copy(pout.at[t, 0], pin.at[a, core], p_recv.at[a, core])
        side = pltpu.make_async_remote_copy(
            src_ref=pout.at[t, 1], dst_ref=pin.at[a, core], send_sem=p_send.at[t, 1],
            recv_sem=p_recv.at[a, core], device_id=(origin, sib), device_id_type=MESH,
        )
        pl.when(origin != a)(away.start)
        pl.when(origin == a)(here.start)
        side.start()
        sends.append((origin, away, side))

    for row in range(rows_of):
        for s in range(2):
            pltpu.make_async_copy(pout.at[0, 0], pin.at[row, s], p_recv.at[row, s]).wait()
    for s in range(2):
        total = pin[0, s].astype(jnp.float32)
        for row in range(1, rows_of):
            total += pin[row, s].astype(jnp.float32)
        mixed = (total * (K * rows_of) ** (-0.5)).astype(jnp.bfloat16).astype(jnp.float32)
        scaled = scale_channels(mixed, gain[...]).astype(jnp.bfloat16)
        out = jnp.dot(scaled, wo[...], preferred_element_type=jnp.float32)
        flat[s * half : (s + 1) * half, :] = out * gate[s * half : (s + 1) * half, :]
    for i in range(K):
        o_ref[i] = flat[i * J : (i + 1) * J, :].astype(o_ref.dtype)

    for copy in to_line:
        copy.wait_send()
    for origin, away, side in sends:
        pl.when(origin != a)(away.wait_send)
        side.wait_send()


def kernel_body(rows_of, line_of, pair_state, left_weight, right_weight, mid_gain, out_weight, out_gate):
    K, J, D = pair_state.shape
    N = K * J
    half = J * J
    f32, bf16 = jnp.float32, jnp.bfloat16
    anywhere = pl.BlockSpec(memory_space=pl.ANY)
    dma = pltpu.SemaphoreType.DMA
    return pl.pallas_call(
        functools.partial(kernel, rows_of, line_of),
        out_shape=jax.ShapeDtypeStruct((K, J, D), bf16),
        in_specs=[anywhere] * 6,
        out_specs=pl.BlockSpec(memory_space=pltpu.VMEM),
        scratch_shapes=[
            pltpu.VMEM((K, J, D), bf16),
            pltpu.VMEM((D, D), bf16),
            pltpu.VMEM((D, D), bf16),
            pltpu.VMEM((1, D), f32),
            pltpu.VMEM((D, D), bf16),
            pltpu.VMEM((D, D), bf16),
            pltpu.VMEM((N, D), f32),
            pltpu.VMEM((N, D), bf16),
            pltpu.VMEM((N, D), bf16),
            pltpu.VMEM((line_of, N, D), bf16),
            pltpu.VMEM((N, D), f32),
            pltpu.VMEM((K, 2 * J, D), f32),
            pltpu.VMEM((N, D), f32),
            pltpu.VMEM((line_of, 2, half, D), bf16),
            pltpu.VMEM((rows_of, 2, half, D), bf16),
            dma((6,)), dma, dma, dma((line_of,)), dma((line_of,)), dma((line_of, 2)), dma((rows_of, 2)),
        ],
        compiler_params=pltpu.CompilerParams(
            collective_id=0, has_side_effects=True, vmem_limit_bytes=VMEM_LIMIT
        ),
    )(pair_state, left_weight, right_weight, mid_gain.reshape(1, -1), out_weight, out_gate)


def body(rows_of, columns_of, *arrays):
    K, J, D = arrays[0].shape
    fits = (
        columns_of == 2 * rows_of
        and K == 2 * J
        and arrays[1].shape == (D, D)
        and D % 128 == 0
        and J <= 16
        and (J * J) % 16 == 0
    )
    if fits:
        return kernel_body(rows_of, columns_of // 2, *arrays)
    return plain_body(*arrays)


def solution(mesh):
    placed = (P("pr", "pc", None), P(), P(), P(), P(), P())
    return jax.shard_map(
        functools.partial(body, mesh.shape["pr"], mesh.shape["pc"]),
        mesh=mesh, in_specs=placed, out_specs=P("pr", "pc", None), check_vma=False,
    )
```

```python
import functools

import jax
import jax.numpy as jnp
from jax import lax
from jax.experimental import pallas as pl
from jax.experimental.pallas import tpu as pltpu
from jax.sharding import PartitionSpec as P

PIECES = 3
MESH = pl.DeviceIdType.MESH


def scale_channels(values, channel_gain):
    centred = values - jnp.mean(values, axis=-1, keepdims=True)
    return (
        centred
        * lax.rsqrt(jnp.mean(centred * centred, axis=-1, keepdims=True) + 1e-05)
        * channel_gain
    )


def project_pair(pair_in, left_weight, right_weight):
    left = jnp.einsum("ijc,cd->ijd", pair_in, left_weight, preferred_element_type=jnp.float32)
    right = jnp.einsum("ijc,cd->ijd", pair_in, right_weight, preferred_element_type=jnp.float32)
    return (pair_in, left.astype(jnp.bfloat16), right.astype(jnp.bfloat16))


def close_update(mixed, ready, mid_gain, out_weight, out_gate):
    scaled = scale_channels(mixed.astype(jnp.float32), mid_gain).astype(jnp.bfloat16)
    scaled = lax.optimization_barrier(scaled)
    gate = jax.nn.sigmoid(
        jnp.einsum("ijc,cd->ijd", ready, out_gate, preferred_element_type=jnp.float32)
    )
    return (
        jnp.einsum("ijd,dc->ijc", scaled, out_weight, preferred_element_type=jnp.float32) * gate
    ).astype(jnp.bfloat16)


def plain_body(pair_state, left_weight, right_weight, mid_gain, out_weight, out_gate):
    ready, left, right = project_pair(pair_state, left_weight, right_weight)
    count = pair_state.shape[0] * lax.axis_size("pr")
    left_lines, right_lines = (
        lax.all_to_all(left, "pr", split_axis=2, concat_axis=0, tiled=True),
        lax.all_to_all(right, "pr", split_axis=2, concat_axis=0, tiled=True),
    )
    strip = jnp.einsum(
        "kid,kjd->ijd",
        lax.all_gather(left_lines, "pc", axis=1, tiled=True),
        right_lines,
        preferred_element_type=jnp.float32,
    )
    strip = (strip * count ** (-0.5)).astype(jnp.bfloat16)
    mixed = lax.all_to_all(strip, "pr", split_axis=0, concat_axis=2, tiled=True)
    return close_update(mixed, ready, mid_gain, out_weight, out_gate)


def kernel(
    rows_of, line_of, J,
    x_hbm, wl_hbm, wr_hbm, gain_hbm, wo_hbm, wg_hbm, o_ref,
    xv, wl, wr, gain, wo, wg, xsib, zbuf, lbuf, rflat, rbuf, flat, mixed, gate, pout, pin,
    in_sem, x_send, x_recv, z_send, z_recv, r_send, p_send, p_recv,
):
    N, D = xv.shape[0] * xv.shape[1], xv.shape[2]
    K = N // J
    G = PIECES
    I = J // G
    part = I * J
    a = lax.axis_index("pr")
    c = lax.axis_index("pc")
    z, core = c // 2, c % 2
    sib = c + 1 - 2 * core
    way = 1 - 2 * (z // 2)
    near = z + way
    far = (z - way + line_of) % line_of
    third = (z + 2) % line_of
    middle = ((z + 1) % line_of) // 2 == 1

    barrier = pltpu.get_barrier_semaphore()
    for other in (near, far):
        pl.semaphore_signal(barrier, inc=1, device_id=(a, other * 2 + core), device_id_type=MESH)
    pl.semaphore_signal(barrier, inc=1, device_id=(a, sib), device_id_type=MESH)
    for step in range(1, rows_of):
        row = (a + step) % rows_of
        pl.semaphore_signal(barrier, inc=1, device_id=(row, c), device_id_type=MESH)
        pl.semaphore_signal(barrier, inc=1, device_id=(row, sib), device_id_type=MESH)
    loads = [
        pltpu.make_async_copy(s, d, in_sem.at[n])
        for n, (s, d) in enumerate(
            ((x_hbm, xv), (wr_hbm, wr), (wl_hbm, wl), (wg_hbm, wg), (gain_hbm, gain), (wo_hbm, wo))
        )
    ]
    for load in loads:
        load.start()
    for load in loads:
        load.wait()

    xs = xv[...].reshape(N, D)
    own = jnp.dot(xs, wr[...], preferred_element_type=jnp.float32)
    rflat[:N, :] = own
    lbuf[...] = jnp.dot(xs, wl[...], preferred_element_type=jnp.float32)
    gate[...] = jax.nn.sigmoid(jnp.dot(xs, wg[...], preferred_element_type=jnp.float32))

    pl.semaphore_wait(barrier, 3 + 2 * (rows_of - 1))

    def along(src, origin, g, target, sem):
        return pltpu.make_async_remote_copy(
            src_ref=src, dst_ref=zbuf.at[origin, g], send_sem=sem, recv_sem=z_recv.at[origin, g],
            device_id=(a, target * 2 + core), device_id_type=MESH,
        )

    def arrived(origin, g):
        pltpu.make_async_copy(xv.at[g], zbuf.at[origin, g], z_recv.at[origin, g]).wait()

    sent = []
    for t, target in enumerate((near, far)):
        for g in range(G):
            copy = along(xv.at[g], z, g, target, z_send.at[t, g])
            copy.start()
            sent.append(copy)
    to_sib = pltpu.make_async_remote_copy(
        src_ref=xv, dst_ref=xsib, send_sem=x_send, recv_sem=x_recv,
        device_id=(a, sib), device_id_type=MESH,
    )
    to_sib.start()
    to_sib.wait()
    rflat[N:, :] = jnp.dot(xsib[...].reshape(N, D), wr[...], preferred_element_type=jnp.float32)
    for k in range(K):
        rbuf[k] = rflat[pl.ds(k, 2 * J, stride=K), :]

    sums_sent = []

    def contract(t, origin, g, base):
        def step(k, sums):
            right = rbuf[k]
            return tuple(
                total + lbuf[pl.ds(base + i * K + k, 1), :] * right for i, total in enumerate(sums)
            )

        sums = lax.fori_loop(
            0, K, step, tuple(jnp.zeros((2 * J, D), jnp.float32) for _ in range(I)), unroll=4
        )
        for i in range(I):
            flat[i * J : (i + 1) * J, :] = sums[i][:J]
            flat[part + i * J : part + (i + 1) * J, :] = sums[i][J:]
        for h in range(2):
            pout[t, g, h] = flat[h * part : (h + 1) * part, :].astype(pout.dtype)
        landing, sem = pin.at[g, core, a], p_recv.at[g, core, a]
        away = pltpu.make_async_remote_copy(
            src_ref=pout.at[t, g, 0], dst_ref=landing, send_sem=p_send.at[t, g, 0], recv_sem=sem,
            device_id=(origin, c), device_id_type=MESH,
        )
        here = pltpu.make_async_copy(pout.at[t, g, 0], landing, sem)
        side = pltpu.make_async_remote_copy(
            src_ref=pout.at[t, g, 1], dst_ref=landing, send_sem=p_send.at[t, g, 1], recv_sem=sem,
            device_id=(origin, sib), device_id_type=MESH,
        )
        pl.when(origin != a)(away.start)
        pl.when(origin == a)(here.start)
        side.start()
        sums_sent.append((origin, away, side))

    def project(origin, g):
        block = zbuf[origin, g]
        lbuf[: I * K, :] = jnp.dot(block, wl[...], preferred_element_type=jnp.float32)

    for g in range(G):
        contract(0, z, g, g * I * K)
    relays = []
    for g in range(G):
        arrived(near, g)
        first = along(zbuf.at[near, g], near, g, far, r_send.at[0, g])
        second = along(zbuf.at[far, g], far, g, near, r_send.at[1, g])
        relays += [first, second]

        @pl.when(middle)
        def _():
            first.start()
            arrived(far, g)
            second.start()

        project(near, g)
        contract(1, near, g, 0)
    for g in range(G):

        @pl.when(jnp.logical_not(middle))
        def _():
            arrived(far, g)

        project(far, g)
        contract(2, far, g, 0)
        arrived(third, g)
        project(third, g)
        contract(3, third, g, 0)

    for g in range(G):
        totals = []
        for s in range(2):
            for row in range(rows_of):
                pltpu.make_async_copy(pout.at[0, 0, 0], pin.at[g, s, row], p_recv.at[g, s, row]).wait()
            total = pin[g, s, 0].astype(jnp.float32)
            for row in range(1, rows_of):
                total += pin[g, s, row].astype(jnp.float32)
            totals.append(total)
        total = jnp.concatenate(totals, axis=0) * (K * rows_of) ** (-0.5)
        total = total.astype(jnp.bfloat16).astype(jnp.float32)
        scaled = scale_channels(total, gain[...]).astype(jnp.bfloat16)
        out = jnp.dot(scaled, wo[...], preferred_element_type=jnp.float32)
        for s in range(2):
            for i in range(I):
                first_row = s * part + i * J
                mixed[pl.ds((s * G + g) * I + i, J, stride=K), :] = out[first_row : first_row + J]
    o_ref[...] = (mixed[...] * gate[...]).astype(o_ref.dtype)

    for copy in sent:
        copy.wait_send()

    @pl.when(middle)
    def _():
        for copy in relays:
            copy.wait_send()

    for origin, away, side in sums_sent:
        pl.when(origin != a)(away.wait_send)
        side.wait_send()


def kernel_body(rows_of, line_of, pair_state, left_weight, right_weight, mid_gain, out_weight, out_gate):
    K, J, D = pair_state.shape
    N = K * J
    G = PIECES
    I = J // G
    f32, bf16 = jnp.float32, jnp.bfloat16
    anywhere = pl.BlockSpec(memory_space=pl.ANY)
    dma = pltpu.SemaphoreType.DMA
    pieces = jnp.transpose(pair_state, (1, 0, 2)).reshape(G, I * K, D)
    update = pl.pallas_call(
        functools.partial(kernel, rows_of, line_of, J),
        out_shape=jax.ShapeDtypeStruct((N, D), bf16),
        in_specs=[anywhere] * 6,
        out_specs=pl.BlockSpec(memory_space=pltpu.VMEM),
        scratch_shapes=[
            pltpu.VMEM((G, I * K, D), bf16),
            pltpu.VMEM((D, D), bf16),
            pltpu.VMEM((D, D), bf16),
            pltpu.VMEM((1, D), f32),
            pltpu.VMEM((D, D), bf16),
            pltpu.VMEM((D, D), bf16),
            pltpu.VMEM((G, I * K, D), bf16),
            pltpu.VMEM((line_of, G, I * K, D), bf16),
            pltpu.VMEM((N, D), f32),
            pltpu.VMEM((2 * N, D), f32),
            pltpu.VMEM((K, 2 * J, D), f32),
            pltpu.VMEM((2 * I * J, D), f32),
            pltpu.VMEM((N, D), f32),
            pltpu.VMEM((N, D), f32),
            pltpu.VMEM((line_of, G, 2, I * J, D), bf16),
            pltpu.VMEM((G, 2, rows_of, I * J, D), bf16),
            dma((6,)), dma, dma, dma((2, G)), dma((line_of, G)), dma((2, G)),
            dma((line_of, G, 2)), dma((G, 2, rows_of)),
        ],
        compiler_params=pltpu.CompilerParams(collective_id=0, has_side_effects=True),
    )(pieces, left_weight, right_weight, mid_gain.reshape(1, -1), out_weight, out_gate)
    return jnp.transpose(update.reshape(J, K, D), (1, 0, 2))


def body(rows_of, columns_of, *arrays):
    K, J, D = arrays[0].shape
    fits = (
        columns_of == 2 * rows_of
        and columns_of == 8
        and K == 2 * J
        and arrays[1].shape == (D, D)
        and D % 128 == 0
        and J <= 16
        and J % PIECES == 0
    )
    if fits:
        return kernel_body(rows_of, columns_of // 2, *arrays)
    return plain_body(*arrays)


def solution(mesh):
    placed = (P("pr", "pc", None), P(), P(), P(), P(), P())
    return jax.shard_map(
        functools.partial(body, mesh.shape["pr"], mesh.shape["pc"]),
        mesh=mesh, in_specs=placed, out_specs=P("pr", "pc", None), check_vma=False,
    )
```

```python
import functools

import jax
import jax.numpy as jnp
from jax import lax
from jax.experimental import pallas as pl
from jax.experimental.pallas import tpu as pltpu
from jax.sharding import PartitionSpec as P

PIECES = 2
MESH = pl.DeviceIdType.MESH


def scale_channels(values, channel_gain):
    centred = values - jnp.mean(values, axis=-1, keepdims=True)
    return (
        centred
        * lax.rsqrt(jnp.mean(centred * centred, axis=-1, keepdims=True) + 1e-05)
        * channel_gain
    )


def project_pair(pair_in, left_weight, right_weight):
    left = jnp.einsum("ijc,cd->ijd", pair_in, left_weight, preferred_element_type=jnp.float32)
    right = jnp.einsum("ijc,cd->ijd", pair_in, right_weight, preferred_element_type=jnp.float32)
    return (pair_in, left.astype(jnp.bfloat16), right.astype(jnp.bfloat16))


def close_update(mixed, ready, mid_gain, out_weight, out_gate):
    scaled = scale_channels(mixed.astype(jnp.float32), mid_gain).astype(jnp.bfloat16)
    scaled = lax.optimization_barrier(scaled)
    gate = jax.nn.sigmoid(
        jnp.einsum("ijc,cd->ijd", ready, out_gate, preferred_element_type=jnp.float32)
    )
    return (
        jnp.einsum("ijd,dc->ijc", scaled, out_weight, preferred_element_type=jnp.float32) * gate
    ).astype(jnp.bfloat16)


def plain_body(pair_state, left_weight, right_weight, mid_gain, out_weight, out_gate):
    ready, left, right = project_pair(pair_state, left_weight, right_weight)
    count = pair_state.shape[0] * lax.axis_size("pr")
    left_lines, right_lines = (
        lax.all_to_all(left, "pr", split_axis=2, concat_axis=0, tiled=True),
        lax.all_to_all(right, "pr", split_axis=2, concat_axis=0, tiled=True),
    )
    strip = jnp.einsum(
        "kid,kjd->ijd",
        lax.all_gather(left_lines, "pc", axis=1, tiled=True),
        right_lines,
        preferred_element_type=jnp.float32,
    )
    strip = (strip * count ** (-0.5)).astype(jnp.bfloat16)
    mixed = lax.all_to_all(strip, "pr", split_axis=0, concat_axis=2, tiled=True)
    return close_update(mixed, ready, mid_gain, out_weight, out_gate)


def kernel(
    rows_of, line_of, J,
    x_hbm, wl_hbm, wr_hbm, gain_hbm, wo_hbm, wg_hbm, o_ref,
    xv, wl, wr, gain, wo, wg, xsib, zbuf, lbuf, rflat, rbuf, flat, mixed, gate, pout, pin,
    in_sem, x_send, x_recv, z_send, z_recv, r_send, p_send, p_recv, ready, ends,
):
    N, D = xv.shape[0] * xv.shape[1], xv.shape[2]
    K = N // J
    G = PIECES
    I = J // G
    part = I * J
    a = lax.axis_index("pr")
    c = lax.axis_index("pc")
    z, core = c // 2, c % 2
    sib = c + 1 - 2 * core
    way = 1 - 2 * (z // 2)
    inner = ((z + 1) % line_of) // 2
    middle = inner == 1
    near = z + way
    far = (z - way + line_of) % line_of
    third = (z + 2) % line_of
    across = a + 1 - 2 * (a % 2)
    along_y = (a + 2) % rows_of

    barrier = pltpu.get_barrier_semaphore()

    def greet(row, column):
        pl.semaphore_signal(barrier, inc=1, device_id=(row, column), device_id_type=MESH)

    greet(a, near * 2 + core)
    pl.when(middle)(lambda: greet(a, far * 2 + core))
    for row in (across, along_y):
        greet(row, c)
        greet(row, sib)
    greet(a, sib)
    loads = [
        pltpu.make_async_copy(s, d, in_sem.at[n])
        for n, (s, d) in enumerate(
            ((x_hbm, xv), (wr_hbm, wr), (wl_hbm, wl), (wg_hbm, wg), (gain_hbm, gain), (wo_hbm, wo))
        )
    ]
    for load in loads:
        load.start()
    for load in loads:
        load.wait()

    xs = xv[...].reshape(N, D)
    own = jnp.dot(xs, wr[...], preferred_element_type=jnp.float32)
    rflat[:N, :] = own
    lbuf[...] = jnp.dot(xs, wl[...], preferred_element_type=jnp.float32)
    gate[...] = jax.nn.sigmoid(jnp.dot(xs, wg[...], preferred_element_type=jnp.float32))

    pl.semaphore_wait(barrier, 6 + inner)

    def along(src, origin, g, target, sem):
        return pltpu.make_async_remote_copy(
            src_ref=src, dst_ref=zbuf.at[origin, g], send_sem=sem, recv_sem=z_recv.at[origin, g],
            device_id=(a, target * 2 + core), device_id_type=MESH,
        )

    def arrived(origin, g):
        pltpu.make_async_copy(xv.at[g], zbuf.at[origin, g], z_recv.at[origin, g]).wait()

    to_sib = pltpu.make_async_remote_copy(
        src_ref=xv, dst_ref=xsib, send_sem=x_send, recv_sem=x_recv,
        device_id=(a, sib), device_id_type=MESH,
    )
    to_sib.start()
    outward = [along(xv.at[g], z, g, far, z_send.at[1, g]) for g in range(G)]
    sent = [along(xv.at[g], z, g, near, z_send.at[0, g]) for g in range(G)]
    for copy in sent:
        copy.start()

    pl.semaphore_signal(ready, inc=1, device_id=(across, c), device_id_type=MESH)

    @pl.when(middle)
    def _():
        pl.semaphore_signal(ends, inc=1, device_id=(a, near * 2 + core), device_id_type=MESH)
        for copy in outward:
            copy.start()
        pl.semaphore_wait(ends, 1)
        pl.semaphore_signal(ends, inc=1, device_id=(a, far * 2 + core), device_id_type=MESH)

    @pl.when(jnp.logical_not(middle))
    def _():
        pl.semaphore_wait(ends, 1)
        for copy in outward:
            copy.start()

    to_sib.wait()
    rflat[N:, :] = jnp.dot(xsib[...].reshape(N, D), wr[...], preferred_element_type=jnp.float32)
    for k in range(K):
        rbuf[k] = rflat[pl.ds(k, 2 * J, stride=K), :]

    sums_sent = []

    def contract(t, origin, g, base):
        def step(k, sums):
            right = rbuf[k]
            return tuple(
                total + lbuf[pl.ds(base + i * K + k, 1), :] * right for i, total in enumerate(sums)
            )

        sums = lax.fori_loop(
            0, K, step, tuple(jnp.zeros((2 * J, D), jnp.float32) for _ in range(I)), unroll=4
        )
        for i in range(I):
            flat[i * J : (i + 1) * J, :] = sums[i][:J]
            flat[part + i * J : part + (i + 1) * J, :] = sums[i][J:]
        for h in range(2):
            pout[t, g, h] = flat[h * part : (h + 1) * part, :].astype(pout.dtype)
        landing, sem = pin.at[g, core, a], p_recv.at[g, core, a]
        away = pltpu.make_async_remote_copy(
            src_ref=pout.at[t, g, 0], dst_ref=landing, send_sem=p_send.at[t, g, 0], recv_sem=sem,
            device_id=(origin, c), device_id_type=MESH,
        )
        here = pltpu.make_async_copy(pout.at[t, g, 0], landing, sem)
        side = pltpu.make_async_remote_copy(
            src_ref=pout.at[t, g, 1], dst_ref=landing, send_sem=p_send.at[t, g, 1], recv_sem=sem,
            device_id=(origin, sib), device_id_type=MESH,
        )
        pl.when(origin != a)(away.start)
        pl.when(origin == a)(here.start)
        side.start()
        sums_sent.append((origin, away, side))

    def project(origin, g):
        block = zbuf[origin, g]
        lbuf[: I * K, :] = jnp.dot(block, wl[...], preferred_element_type=jnp.float32)

    pl.semaphore_wait(ready, 1)
    for g in range(G):
        contract(0, z, g, g * I * K)
    relays = []
    for g in range(G):
        arrived(near, g)
        first = along(zbuf.at[near, g], near, g, far, r_send.at[0, g])
        second = along(zbuf.at[far, g], far, g, near, r_send.at[1, g])
        relays += [first, second]

        @pl.when(middle)
        def _():
            first.start()
            arrived(far, g)
            second.start()

        project(near, g)
        contract(1, near, g, 0)
    for g in range(G):

        @pl.when(jnp.logical_not(middle))
        def _():
            arrived(far, g)

        project(far, g)
        contract(2, far, g, 0)
        arrived(third, g)
        project(third, g)
        contract(3, third, g, 0)

    for g in range(G):
        totals = []
        for s in range(2):
            for row in range(rows_of):
                pltpu.make_async_copy(pout.at[0, 0, 0], pin.at[g, s, row], p_recv.at[g, s, row]).wait()
            total = pin[g, s, 0].astype(jnp.float32)
            for row in range(1, rows_of):
                total += pin[g, s, row].astype(jnp.float32)
            totals.append(total)
        total = jnp.concatenate(totals, axis=0) * (K * rows_of) ** (-0.5)
        total = total.astype(jnp.bfloat16).astype(jnp.float32)
        scaled = scale_channels(total, gain[...]).astype(jnp.bfloat16)
        out = jnp.dot(scaled, wo[...], preferred_element_type=jnp.float32)
        for s in range(2):
            for i in range(I):
                first_row = s * part + i * J
                mixed[pl.ds((s * G + g) * I + i, J, stride=K), :] = out[first_row : first_row + J]
    o_ref[...] = (mixed[...] * gate[...]).astype(o_ref.dtype)

    for copy in sent:
        copy.wait_send()

    for copy in outward:
        copy.wait_send()

    @pl.when(middle)
    def _():
        for copy in relays:
            copy.wait_send()

    for origin, away, side in sums_sent:
        pl.when(origin != a)(away.wait_send)
        side.wait_send()


def kernel_body(rows_of, line_of, pair_state, left_weight, right_weight, mid_gain, out_weight, out_gate):
    K, J, D = pair_state.shape
    N = K * J
    G = PIECES
    I = J // G
    f32, bf16 = jnp.float32, jnp.bfloat16
    anywhere = pl.BlockSpec(memory_space=pl.ANY)
    dma = pltpu.SemaphoreType.DMA
    pieces = jnp.transpose(pair_state, (1, 0, 2)).reshape(G, I * K, D)
    update = pl.pallas_call(
        functools.partial(kernel, rows_of, line_of, J),
        out_shape=jax.ShapeDtypeStruct((N, D), bf16),
        in_specs=[anywhere] * 6,
        out_specs=pl.BlockSpec(memory_space=pltpu.VMEM),
        scratch_shapes=[
            pltpu.VMEM((G, I * K, D), bf16),
            pltpu.VMEM((D, D), bf16),
            pltpu.VMEM((D, D), bf16),
            pltpu.VMEM((1, D), f32),
            pltpu.VMEM((D, D), bf16),
            pltpu.VMEM((D, D), bf16),
            pltpu.VMEM((G, I * K, D), bf16),
            pltpu.VMEM((line_of, G, I * K, D), bf16),
            pltpu.VMEM((N, D), f32),
            pltpu.VMEM((2 * N, D), f32),
            pltpu.VMEM((K, 2 * J, D), f32),
            pltpu.VMEM((2 * I * J, D), f32),
            pltpu.VMEM((N, D), f32),
            pltpu.VMEM((N, D), f32),
            pltpu.VMEM((line_of, G, 2, I * J, D), bf16),
            pltpu.VMEM((G, 2, rows_of, I * J, D), bf16),
            dma((6,)), dma, dma, dma((2, G)), dma((line_of, G)), dma((2, G)),
            dma((line_of, G, 2)), dma((G, 2, rows_of)), pltpu.SemaphoreType.REGULAR,
            pltpu.SemaphoreType.REGULAR,
        ],
        compiler_params=pltpu.CompilerParams(collective_id=0, has_side_effects=True),
    )(pieces, left_weight, right_weight, mid_gain.reshape(1, -1), out_weight, out_gate)
    return jnp.transpose(update.reshape(J, K, D), (1, 0, 2))


def body(rows_of, columns_of, *arrays):
    K, J, D = arrays[0].shape
    fits = (
        columns_of == 2 * rows_of
        and columns_of == 8
        and K == 2 * J
        and arrays[1].shape == (D, D)
        and D % 128 == 0
        and J <= 16
        and J % PIECES == 0
    )
    if fits:
        return kernel_body(rows_of, columns_of // 2, *arrays)
    return plain_body(*arrays)


def solution(mesh):
    placed = (P("pr", "pc", None), P(), P(), P(), P(), P())
    return jax.shard_map(
        functools.partial(body, mesh.shape["pr"], mesh.shape["pc"]),
        mesh=mesh, in_specs=placed, out_specs=P("pr", "pc", None), check_vma=False,
    )
```

```python
import functools

import jax
import jax.numpy as jnp
from jax import lax
from jax.experimental import pallas as pl
from jax.experimental.pallas import tpu as pltpu
from jax.sharding import PartitionSpec as P

PIECES = 2
MESH = pl.DeviceIdType.MESH


def scale_channels(values, channel_gain):
    centred = values - jnp.mean(values, axis=-1, keepdims=True)
    return (
        centred
        * lax.rsqrt(jnp.mean(centred * centred, axis=-1, keepdims=True) + 1e-05)
        * channel_gain
    )


def project_pair(pair_in, left_weight, right_weight):
    left = jnp.einsum("ijc,cd->ijd", pair_in, left_weight, preferred_element_type=jnp.float32)
    right = jnp.einsum("ijc,cd->ijd", pair_in, right_weight, preferred_element_type=jnp.float32)
    return (pair_in, left.astype(jnp.bfloat16), right.astype(jnp.bfloat16))


def close_update(mixed, ready, mid_gain, out_weight, out_gate):
    scaled = scale_channels(mixed.astype(jnp.float32), mid_gain).astype(jnp.bfloat16)
    scaled = lax.optimization_barrier(scaled)
    gate = jax.nn.sigmoid(
        jnp.einsum("ijc,cd->ijd", ready, out_gate, preferred_element_type=jnp.float32)
    )
    return (
        jnp.einsum("ijd,dc->ijc", scaled, out_weight, preferred_element_type=jnp.float32) * gate
    ).astype(jnp.bfloat16)


def plain_body(pair_state, left_weight, right_weight, mid_gain, out_weight, out_gate):
    ready, left, right = project_pair(pair_state, left_weight, right_weight)
    count = pair_state.shape[0] * lax.axis_size("pr")
    left_lines, right_lines = (
        lax.all_to_all(left, "pr", split_axis=2, concat_axis=0, tiled=True),
        lax.all_to_all(right, "pr", split_axis=2, concat_axis=0, tiled=True),
    )
    strip = jnp.einsum(
        "kid,kjd->ijd",
        lax.all_gather(left_lines, "pc", axis=1, tiled=True),
        right_lines,
        preferred_element_type=jnp.float32,
    )
    strip = (strip * count ** (-0.5)).astype(jnp.bfloat16)
    mixed = lax.all_to_all(strip, "pr", split_axis=0, concat_axis=2, tiled=True)
    return close_update(mixed, ready, mid_gain, out_weight, out_gate)


def kernel(
    rows_of, line_of, J,
    x_hbm, wl_hbm, wr_hbm, gain_hbm, wo_hbm, wg_hbm, o_ref,
    xv, wl, wr, gain, wo, wg, xsib, zbuf, lbuf, rflat, rbuf, flat, mixed, gate, pout, pin,
    in_sem, x_send, x_recv, z_send, z_recv, r_send, p_send, p_recv, ready, ends,
):
    N, D = xv.shape[0] * xv.shape[1], xv.shape[2]
    K = N // J
    G = PIECES
    I = J // G
    part = I * J
    a = lax.axis_index("pr")
    c = lax.axis_index("pc")
    z, core = c // 2, c % 2
    sib = c + 1 - 2 * core
    way = 1 - 2 * (z // 2)
    inner = ((z + 1) % line_of) // 2
    middle = inner == 1
    near = z + way
    far = (z - way + line_of) % line_of
    third = (z + 2) % line_of
    across = a + 1 - 2 * (a % 2)
    along_y = (a + 2) % rows_of

    barrier = pltpu.get_barrier_semaphore()

    def greet(row, column):
        pl.semaphore_signal(barrier, inc=1, device_id=(row, column), device_id_type=MESH)

    greet(a, near * 2 + core)
    pl.when(middle)(lambda: greet(a, far * 2 + core))
    for row in (across, along_y):
        greet(row, c)
        greet(row, sib)
    greet(a, sib)
    loads = [
        pltpu.make_async_copy(s, d, in_sem.at[n])
        for n, (s, d) in enumerate(
            ((x_hbm, xv), (wr_hbm, wr), (wl_hbm, wl), (wg_hbm, wg), (gain_hbm, gain), (wo_hbm, wo))
        )
    ]
    for load in loads:
        load.start()
    for load in loads:
        load.wait()

    xs = xv[...].reshape(N, D)
    own = jnp.dot(xs, wr[...], preferred_element_type=jnp.float32)
    rflat[:N, :] = own
    lbuf[...] = jnp.dot(xs, wl[...], preferred_element_type=jnp.float32)
    gate[...] = jax.nn.sigmoid(jnp.dot(xs, wg[...], preferred_element_type=jnp.float32))

    pl.semaphore_wait(barrier, 6 + inner)

    def along(src, origin, g, target, sem):
        return pltpu.make_async_remote_copy(
            src_ref=src, dst_ref=zbuf.at[origin, g], send_sem=sem, recv_sem=z_recv.at[origin, g],
            device_id=(a, target * 2 + core), device_id_type=MESH,
        )

    def arrived(origin, g):
        pltpu.make_async_copy(xv.at[g], zbuf.at[origin, g], z_recv.at[origin, g]).wait()

    to_sib = pltpu.make_async_remote_copy(
        src_ref=xv, dst_ref=xsib, send_sem=x_send, recv_sem=x_recv,
        device_id=(a, sib), device_id_type=MESH,
    )
    to_sib.start()
    outward = [along(xv.at[g], z, g, far, z_send.at[1, g]) for g in range(G)]
    sent = [along(xv.at[g], z, g, near, z_send.at[0, g]) for g in range(G)]
    for copy in sent:
        copy.start()

    pl.semaphore_signal(ready, inc=1, device_id=(across, c), device_id_type=MESH)

    @pl.when(middle)
    def _():
        pl.semaphore_signal(ends, inc=1, device_id=(a, near * 2 + core), device_id_type=MESH)
        for copy in outward:
            copy.start()
        pl.semaphore_wait(ends, 1)
        pl.semaphore_signal(ends, inc=1, device_id=(a, far * 2 + core), device_id_type=MESH)

    @pl.when(jnp.logical_not(middle))
    def _():
        pl.semaphore_wait(ends, 1)
        for copy in outward:
            copy.start()

    to_sib.wait()
    rflat[N:, :] = jnp.dot(xsib[...].reshape(N, D), wr[...], preferred_element_type=jnp.float32)
    for k in range(K):
        rbuf[k] = rflat[pl.ds(k, 2 * J, stride=K), :]

    sums_sent = []

    def contract(t, origin, g, base):
        def step(k, sums):
            right = rbuf[k]
            return tuple(
                total + lbuf[pl.ds(base + i * K + k, 1), :] * right for i, total in enumerate(sums)
            )

        sums = lax.fori_loop(
            0, K, step, tuple(jnp.zeros((2 * J, D), jnp.float32) for _ in range(I)), unroll=K
        )
        for i in range(I):
            flat[i * J : (i + 1) * J, :] = sums[i][:J]
            flat[part + i * J : part + (i + 1) * J, :] = sums[i][J:]
        for h in range(2):
            pout[t, g, h] = flat[h * part : (h + 1) * part, :].astype(pout.dtype)
        landing, sem = pin.at[g, core, a], p_recv.at[g, core, a]
        away = pltpu.make_async_remote_copy(
            src_ref=pout.at[t, g, 0], dst_ref=landing, send_sem=p_send.at[t, g, 0], recv_sem=sem,
            device_id=(origin, c), device_id_type=MESH,
        )
        here = pltpu.make_async_copy(pout.at[t, g, 0], landing, sem)
        side = pltpu.make_async_remote_copy(
            src_ref=pout.at[t, g, 1], dst_ref=landing, send_sem=p_send.at[t, g, 1], recv_sem=sem,
            device_id=(origin, sib), device_id_type=MESH,
        )
        pl.when(origin != a)(away.start)
        pl.when(origin == a)(here.start)
        side.start()
        sums_sent.append((origin, away, side))

    def project(origin, g):
        block = zbuf[origin, g]
        lbuf[: I * K, :] = jnp.dot(block, wl[...], preferred_element_type=jnp.float32)

    pl.semaphore_wait(ready, 1)
    for g in range(G):
        contract(0, z, g, g * I * K)
    relays = []
    for g in range(G):
        arrived(near, g)
        first = along(zbuf.at[near, g], near, g, far, r_send.at[0, g])
        second = along(zbuf.at[far, g], far, g, near, r_send.at[1, g])
        relays += [first, second]

        @pl.when(middle)
        def _():
            first.start()
            arrived(far, g)
            second.start()

    for g in range(G):
        project(near, g)
        contract(1, near, g, 0)
    for g in range(G):

        @pl.when(jnp.logical_not(middle))
        def _():
            arrived(far, g)

        project(far, g)
        contract(2, far, g, 0)
        arrived(third, g)
        project(third, g)
        contract(3, third, g, 0)

    for g in range(G):
        totals = []
        for s in range(2):
            for row in range(rows_of):
                pltpu.make_async_copy(pout.at[0, 0, 0], pin.at[g, s, row], p_recv.at[g, s, row]).wait()
            total = pin[g, s, 0].astype(jnp.float32)
            for row in range(1, rows_of):
                total += pin[g, s, row].astype(jnp.float32)
            totals.append(total)
        total = jnp.concatenate(totals, axis=0) * (K * rows_of) ** (-0.5)
        total = total.astype(jnp.bfloat16).astype(jnp.float32)
        scaled = scale_channels(total, gain[...]).astype(jnp.bfloat16)
        out = jnp.dot(scaled, wo[...], preferred_element_type=jnp.float32)
        for s in range(2):
            for i in range(I):
                first_row = s * part + i * J
                mixed[pl.ds((s * G + g) * I + i, J, stride=K), :] = out[first_row : first_row + J]
    o_ref[...] = (mixed[...] * gate[...]).astype(o_ref.dtype)

    for copy in sent:
        copy.wait_send()

    for copy in outward:
        copy.wait_send()

    @pl.when(middle)
    def _():
        for copy in relays:
            copy.wait_send()

    for origin, away, side in sums_sent:
        pl.when(origin != a)(away.wait_send)
        side.wait_send()


def kernel_body(rows_of, line_of, pair_state, left_weight, right_weight, mid_gain, out_weight, out_gate):
    K, J, D = pair_state.shape
    N = K * J
    G = PIECES
    I = J // G
    f32, bf16 = jnp.float32, jnp.bfloat16
    anywhere = pl.BlockSpec(memory_space=pl.ANY)
    dma = pltpu.SemaphoreType.DMA
    pieces = jnp.transpose(pair_state, (1, 0, 2)).reshape(G, I * K, D)
    update = pl.pallas_call(
        functools.partial(kernel, rows_of, line_of, J),
        out_shape=jax.ShapeDtypeStruct((N, D), bf16),
        in_specs=[anywhere] * 6,
        out_specs=pl.BlockSpec(memory_space=pltpu.VMEM),
        scratch_shapes=[
            pltpu.VMEM((G, I * K, D), bf16),
            pltpu.VMEM((D, D), bf16),
            pltpu.VMEM((D, D), bf16),
            pltpu.VMEM((1, D), f32),
            pltpu.VMEM((D, D), bf16),
            pltpu.VMEM((D, D), bf16),
            pltpu.VMEM((G, I * K, D), bf16),
            pltpu.VMEM((line_of, G, I * K, D), bf16),
            pltpu.VMEM((N, D), f32),
            pltpu.VMEM((2 * N, D), f32),
            pltpu.VMEM((K, 2 * J, D), f32),
            pltpu.VMEM((2 * I * J, D), f32),
            pltpu.VMEM((N, D), f32),
            pltpu.VMEM((N, D), f32),
            pltpu.VMEM((line_of, G, 2, I * J, D), bf16),
            pltpu.VMEM((G, 2, rows_of, I * J, D), bf16),
            dma((6,)), dma, dma, dma((2, G)), dma((line_of, G)), dma((2, G)),
            dma((line_of, G, 2)), dma((G, 2, rows_of)), pltpu.SemaphoreType.REGULAR,
            pltpu.SemaphoreType.REGULAR,
        ],
        compiler_params=pltpu.CompilerParams(collective_id=0, has_side_effects=True),
    )(pieces, left_weight, right_weight, mid_gain.reshape(1, -1), out_weight, out_gate)
    return jnp.transpose(update.reshape(J, K, D), (1, 0, 2))


def body(rows_of, columns_of, *arrays):
    K, J, D = arrays[0].shape
    fits = (
        columns_of == 2 * rows_of
        and columns_of == 8
        and K == 2 * J
        and arrays[1].shape == (D, D)
        and D % 128 == 0
        and J <= 16
        and J % PIECES == 0
    )
    if fits:
        return kernel_body(rows_of, columns_of // 2, *arrays)
    return plain_body(*arrays)


def solution(mesh):
    placed = (P("pr", "pc", None), P(), P(), P(), P(), P())
    return jax.shard_map(
        functools.partial(body, mesh.shape["pr"], mesh.shape["pc"]),
        mesh=mesh, in_specs=placed, out_specs=P("pr", "pc", None), check_vma=False,
    )
```

```python
import functools

import jax
import jax.numpy as jnp
from jax import lax
from jax.experimental import pallas as pl
from jax.experimental.pallas import tpu as pltpu
from jax.sharding import PartitionSpec as P

PIECES = 2
MESH = pl.DeviceIdType.MESH


def scale_channels(values, channel_gain):
    centred = values - jnp.mean(values, axis=-1, keepdims=True)
    return (
        centred
        * lax.rsqrt(jnp.mean(centred * centred, axis=-1, keepdims=True) + 1e-05)
        * channel_gain
    )


def project_pair(pair_in, left_weight, right_weight):
    left = jnp.einsum("ijc,cd->ijd", pair_in, left_weight, preferred_element_type=jnp.float32)
    right = jnp.einsum("ijc,cd->ijd", pair_in, right_weight, preferred_element_type=jnp.float32)
    return (pair_in, left.astype(jnp.bfloat16), right.astype(jnp.bfloat16))


def close_update(mixed, ready, mid_gain, out_weight, out_gate):
    scaled = scale_channels(mixed.astype(jnp.float32), mid_gain).astype(jnp.bfloat16)
    scaled = lax.optimization_barrier(scaled)
    gate = jax.nn.sigmoid(
        jnp.einsum("ijc,cd->ijd", ready, out_gate, preferred_element_type=jnp.float32)
    )
    return (
        jnp.einsum("ijd,dc->ijc", scaled, out_weight, preferred_element_type=jnp.float32) * gate
    ).astype(jnp.bfloat16)


def plain_body(pair_state, left_weight, right_weight, mid_gain, out_weight, out_gate):
    ready, left, right = project_pair(pair_state, left_weight, right_weight)
    count = pair_state.shape[0] * lax.axis_size("pr")
    left_lines, right_lines = (
        lax.all_to_all(left, "pr", split_axis=2, concat_axis=0, tiled=True),
        lax.all_to_all(right, "pr", split_axis=2, concat_axis=0, tiled=True),
    )
    strip = jnp.einsum(
        "kid,kjd->ijd",
        lax.all_gather(left_lines, "pc", axis=1, tiled=True),
        right_lines,
        preferred_element_type=jnp.float32,
    )
    strip = (strip * count ** (-0.5)).astype(jnp.bfloat16)
    mixed = lax.all_to_all(strip, "pr", split_axis=0, concat_axis=2, tiled=True)
    return close_update(mixed, ready, mid_gain, out_weight, out_gate)


def kernel(
    rows_of, line_of, J,
    x_hbm, wl_hbm, wr_hbm, gain_hbm, wo_hbm, wg_hbm, o_ref,
    xv, wl, wr, gain, wo, wg, xsib, zbuf, lbuf, rflat, rbuf, flat, mixed, gate, pout, pin,
    in_sem, x_send, x_recv, z_send, z_recv, r_send, p_send, p_recv, ready, ends,
):
    N, D = xv.shape[0] * xv.shape[1], xv.shape[2]
    K = N // J
    G = PIECES
    I = J // G
    part = I * J
    a = lax.axis_index("pr")
    c = lax.axis_index("pc")
    z, core = c // 2, c % 2
    sib = c + 1 - 2 * core
    way = 1 - 2 * (z // 2)
    inner = ((z + 1) % line_of) // 2
    middle = inner == 1
    near = z + way
    far = (z - way + line_of) % line_of
    third = (z + 2) % line_of
    across = a + 1 - 2 * (a % 2)
    along_y = (a + 2) % rows_of

    barrier = pltpu.get_barrier_semaphore()

    def greet(row, column):
        pl.semaphore_signal(barrier, inc=1, device_id=(row, column), device_id_type=MESH)

    greet(a, near * 2 + core)
    pl.when(middle)(lambda: greet(a, far * 2 + core))
    for row in (across, along_y):
        greet(row, c)
        greet(row, sib)
    greet(a, sib)
    loads = [
        pltpu.make_async_copy(s, d, in_sem.at[n])
        for n, (s, d) in enumerate(
            ((x_hbm, xv), (wr_hbm, wr), (wl_hbm, wl), (wg_hbm, wg), (gain_hbm, gain), (wo_hbm, wo))
        )
    ]
    for load in loads:
        load.start()
    for load in loads:
        load.wait()

    xs = xv[...].reshape(N, D)
    own = jnp.dot(xs, wr[...], preferred_element_type=jnp.float32)
    rflat[:N, :] = own
    lbuf[...] = jnp.dot(xs, wl[...], preferred_element_type=jnp.float32)
    gate[...] = jax.nn.sigmoid(jnp.dot(xs, wg[...], preferred_element_type=jnp.float32))

    pl.semaphore_wait(barrier, 6 + inner)

    def along(src, origin, g, target, sem):
        return pltpu.make_async_remote_copy(
            src_ref=src, dst_ref=zbuf.at[origin, g], send_sem=sem, recv_sem=z_recv.at[origin, g],
            device_id=(a, target * 2 + core), device_id_type=MESH,
        )

    def arrived(origin, g):
        pltpu.make_async_copy(xv.at[g], zbuf.at[origin, g], z_recv.at[origin, g]).wait()

    to_sib = pltpu.make_async_remote_copy(
        src_ref=xv, dst_ref=xsib, send_sem=x_send, recv_sem=x_recv,
        device_id=(a, sib), device_id_type=MESH,
    )
    to_sib.start()
    outward = [along(xv.at[g], z, g, far, z_send.at[1, g]) for g in range(G)]
    sent = [along(xv.at[g], z, g, near, z_send.at[0, g]) for g in range(G)]
    for copy in sent:
        copy.start()

    pl.semaphore_signal(ready, inc=1, device_id=(across, c), device_id_type=MESH)

    @pl.when(middle)
    def _():
        pl.semaphore_signal(ends, inc=1, device_id=(a, near * 2 + core), device_id_type=MESH)
        for copy in outward:
            copy.start()
        pl.semaphore_wait(ends, 1)
        pl.semaphore_signal(ends, inc=1, device_id=(a, far * 2 + core), device_id_type=MESH)

    @pl.when(jnp.logical_not(middle))
    def _():
        pl.semaphore_wait(ends, 1)
        for copy in outward:
            copy.start()

    to_sib.wait()
    rflat[N:, :] = jnp.dot(xsib[...].reshape(N, D), wr[...], preferred_element_type=jnp.float32)
    for k in range(K):
        rbuf[k] = rflat[pl.ds(k, 2 * J, stride=K), :]

    sums_sent = []

    def contract(t, origin, g, base):
        def step(k, sums):
            right = rbuf[k]
            return tuple(
                total + lbuf[pl.ds(base + i * K + k, 1), :] * right for i, total in enumerate(sums)
            )

        sums = lax.fori_loop(
            0, K, step, tuple(jnp.zeros((2 * J, D), jnp.float32) for _ in range(I)), unroll=K
        )
        for i in range(I):
            flat[i * J : (i + 1) * J, :] = sums[i][:J]
        pout[t, g, 0] = flat[:part, :].astype(pout.dtype)
        landing, sem = pin.at[g, core, a], p_recv.at[g, core, a]
        away = pltpu.make_async_remote_copy(
            src_ref=pout.at[t, g, 0], dst_ref=landing, send_sem=p_send.at[t, g, 0], recv_sem=sem,
            device_id=(origin, c), device_id_type=MESH,
        )
        here = pltpu.make_async_copy(pout.at[t, g, 0], landing, sem)
        side = pltpu.make_async_remote_copy(
            src_ref=pout.at[t, g, 1], dst_ref=landing, send_sem=p_send.at[t, g, 1], recv_sem=sem,
            device_id=(origin, sib), device_id_type=MESH,
        )
        pl.when(origin != a)(away.start)
        pl.when(origin == a)(here.start)
        for i in range(I):
            flat[part + i * J : part + (i + 1) * J, :] = sums[i][J:]
        pout[t, g, 1] = flat[part:, :].astype(pout.dtype)
        side.start()
        sums_sent.append((origin, away, side))

    def project(origin, g):
        block = zbuf[origin, g]
        lbuf[: I * K, :] = jnp.dot(block, wl[...], preferred_element_type=jnp.float32)

    pl.semaphore_wait(ready, 1)
    for g in range(G):
        contract(0, z, g, g * I * K)
    relays = []
    for g in range(G):
        arrived(near, g)
        first = along(zbuf.at[near, g], near, g, far, r_send.at[0, g])
        second = along(zbuf.at[far, g], far, g, near, r_send.at[1, g])
        relays += [first, second]

        @pl.when(middle)
        def _():
            first.start()
            arrived(far, g)
            second.start()

    for g in range(G):
        project(near, g)
        contract(1, near, g, 0)
    for g in range(G):

        @pl.when(jnp.logical_not(middle))
        def _():
            arrived(far, g)

        project(far, g)
        contract(2, far, g, 0)
        arrived(third, g)
        project(third, g)
        contract(3, third, g, 0)

    for g in range(G):
        totals = []
        for s in range(2):
            for row in range(rows_of):
                pltpu.make_async_copy(pout.at[0, 0, 0], pin.at[g, s, row], p_recv.at[g, s, row]).wait()
            total = pin[g, s, 0].astype(jnp.float32)
            for row in range(1, rows_of):
                total += pin[g, s, row].astype(jnp.float32)
            totals.append(total)
        total = jnp.concatenate(totals, axis=0) * (K * rows_of) ** (-0.5)
        total = total.astype(jnp.bfloat16).astype(jnp.float32)
        scaled = scale_channels(total, gain[...]).astype(jnp.bfloat16)
        out = jnp.dot(scaled, wo[...], preferred_element_type=jnp.float32)
        for s in range(2):
            for i in range(I):
                first_row = s * part + i * J
                mixed[pl.ds((s * G + g) * I + i, J, stride=K), :] = out[first_row : first_row + J]
    o_ref[...] = (mixed[...] * gate[...]).astype(o_ref.dtype)

    for copy in sent:
        copy.wait_send()

    for copy in outward:
        copy.wait_send()

    @pl.when(middle)
    def _():
        for copy in relays:
            copy.wait_send()

    for origin, away, side in sums_sent:
        pl.when(origin != a)(away.wait_send)
        side.wait_send()


def kernel_body(rows_of, line_of, pair_state, left_weight, right_weight, mid_gain, out_weight, out_gate):
    K, J, D = pair_state.shape
    N = K * J
    G = PIECES
    I = J // G
    f32, bf16 = jnp.float32, jnp.bfloat16
    anywhere = pl.BlockSpec(memory_space=pl.ANY)
    dma = pltpu.SemaphoreType.DMA
    pieces = jnp.transpose(pair_state, (1, 0, 2)).reshape(G, I * K, D)
    update = pl.pallas_call(
        functools.partial(kernel, rows_of, line_of, J),
        out_shape=jax.ShapeDtypeStruct((N, D), bf16),
        in_specs=[anywhere] * 6,
        out_specs=pl.BlockSpec(memory_space=pltpu.VMEM),
        scratch_shapes=[
            pltpu.VMEM((G, I * K, D), bf16),
            pltpu.VMEM((D, D), bf16),
            pltpu.VMEM((D, D), bf16),
            pltpu.VMEM((1, D), f32),
            pltpu.VMEM((D, D), bf16),
            pltpu.VMEM((D, D), bf16),
            pltpu.VMEM((G, I * K, D), bf16),
            pltpu.VMEM((line_of, G, I * K, D), bf16),
            pltpu.VMEM((N, D), f32),
            pltpu.VMEM((2 * N, D), f32),
            pltpu.VMEM((K, 2 * J, D), f32),
            pltpu.VMEM((2 * I * J, D), f32),
            pltpu.VMEM((N, D), f32),
            pltpu.VMEM((N, D), f32),
            pltpu.VMEM((line_of, G, 2, I * J, D), bf16),
            pltpu.VMEM((G, 2, rows_of, I * J, D), bf16),
            dma((6,)), dma, dma, dma((2, G)), dma((line_of, G)), dma((2, G)),
            dma((line_of, G, 2)), dma((G, 2, rows_of)), pltpu.SemaphoreType.REGULAR,
            pltpu.SemaphoreType.REGULAR,
        ],
        compiler_params=pltpu.CompilerParams(collective_id=0, has_side_effects=True),
    )(pieces, left_weight, right_weight, mid_gain.reshape(1, -1), out_weight, out_gate)
    return jnp.transpose(update.reshape(J, K, D), (1, 0, 2))


def body(rows_of, columns_of, *arrays):
    K, J, D = arrays[0].shape
    fits = (
        columns_of == 2 * rows_of
        and columns_of == 8
        and K == 2 * J
        and arrays[1].shape == (D, D)
        and D % 128 == 0
        and J <= 16
        and J % PIECES == 0
    )
    if fits:
        return kernel_body(rows_of, columns_of // 2, *arrays)
    return plain_body(*arrays)


def solution(mesh):
    placed = (P("pr", "pc", None), P(), P(), P(), P(), P())
    return jax.shard_map(
        functools.partial(body, mesh.shape["pr"], mesh.shape["pc"]),
        mesh=mesh, in_specs=placed, out_specs=P("pr", "pc", None), check_vma=False,
    )
```
